128 devices in a mesh: seq: 64 (over y, z, x), fsdp: 2 (over core).
Axes of the slice: x: 4, y: 4, z: 4, core: 2. Of those that a mesh axis runs over, the one named last changes fastest.
Arguments:
- tokens: bfloat16 [2, 49152, 2560], P('fsdp', 'seq'), may hold values from -6 to 6
- bounds: int32 [2, 64, 2], P('fsdp', 'seq'), may hold values from 0 to 96, as said below
- in_weight: bfloat16 [2560, 5416], P(('seq', 'fsdp')), may hold values from -0.125 to 0.125
- conv_weight: float32 [4, 2816], replicated, may hold values from -0.6 to 0.6
- conv_bias: float32 [2816], replicated, may hold values from -3 to 3
- dt_bias: float32 [40], replicated, may hold values from -4 to 0
- decay_rate: float32 [40], replicated, may hold values from 1.2207031e-05 to 0.5
- skip_gain: float32 [40], replicated, may hold values from 0.1 to 1.9
- norm_gain: float32 [2560], replicated, may hold values from 0.1 to 1.9
Outputs:
- layer_out: bfloat16 [2, 49152, 2560], P('fsdp', 'seq')
The draws below stay inside these ranges and needn't reach their ends.
Inputs may be any that keep to these rules, and one draw needn't show every extreme that they name: For sequence b, bounds[b, s] holds the first and one past the last block of the shard of index s of seq; shards are consecutive in s and cover all 96 blocks; each holds 1 to 3 blocks, and some shard holds 3.
All inputs are finite; a program needn't handle non-finite values.
Results may differ from the reference program's by a relative error of at most 0.0028.
The reference program's roundings to bfloat16 on the way count: a program that leaves them out, or rounds other values in their place, can miss the bound.
Values may be sent and summed in bfloat16 or wider, within the bound.
No kernel may reach another device: no remote copies, remote signals or barrier semaphores. Data moves between devices by JAX's collectives and lax.ppermute only.
A program may use at most 192 MiB of HBM per device.

```python
import jax
import jax.numpy as jnp
from jax import lax

D = 2560
HEADS = 40
HEAD_DIM = 64
STATE = 128
CONV = 4
BLOCK = 256
SLOT_BLOCKS = 3
INNER = 2560
COLS = 5416
SLOTS = 768
TOTAL_BLOCKS = 96
SEQ_LEN = 24576
SEQS = 2
N_SEQ = 64


def draw_bounds(key, part):
    rows = []
    for index in range(SEQS):
        subkey = jax.random.fold_in(key, 11 + index)
        pick_key, order_key = jax.random.split(subkey)
        heavy = jax.random.randint(pick_key, (), 1, N_SEQ // 4 + 1)
        middle = N_SEQ // 2 - 2 * heavy
        ranking = jax.random.permutation(order_key, N_SEQ)
        counts = jnp.where(ranking < heavy, 3, jnp.where(ranking < heavy + middle, 2, 1)).astype(jnp.int32)
        ends = jnp.cumsum(counts).astype(jnp.int32)
        rows.append(jnp.stack([ends - counts, ends], axis=1))
    return jnp.stack(rows).astype(jnp.int32)


def draw_decay_rate(key, part):
    choose_key, value_key = jax.random.split(jax.random.fold_in(key, 5))
    slow_heads = jax.random.uniform(choose_key, (HEADS,)) < 0.5
    spread = jax.random.uniform(value_key, (HEADS,), jnp.float32)
    slow_rate = 0.3 / SEQ_LEN * jnp.exp(spread * jnp.log(10.0))
    fast_rate = 0.05 * jnp.exp(spread * jnp.log(10.0))
    return jnp.where(slow_heads, slow_rate, fast_rate).astype(jnp.float32)


def levels(rng, shape, shards, low, largest):
    gain = 1.0
    for position, shards_of in shards:
        draws = jax.random.uniform(jax.random.fold_in(jax.random.fold_in(rng, 6), position), (shards_of,), jnp.float32, low / len(shards), largest / len(shards))
        gain = gain * jnp.repeat(jnp.exp(draws), shape[position] // shards_of).reshape((-1,) + (1,) * (len(shape) - 1 - position))
    return gain


def noise(stream_key, shape, scale, limit, cuts=(), dtype=jnp.bfloat16):
    array = scale * jax.random.normal(stream_key, shape, jnp.float32)
    if cuts:
        array = array * levels(stream_key, shape, cuts, -0.22, 0.18)
    return jnp.clip(array, -limit, limit).astype(dtype)


def setup_inputs(seed: int = 0) -> dict:
    arg_keys = jax.random.split(jax.random.key(seed), 10)
    tokens = noise(arg_keys[0], (SEQS, N_SEQ * SLOTS, D), 1.0, 6.0, ((0, 2), (1, 64)))
    bounds = draw_bounds(jax.random.fold_in(arg_keys[9], 71), 0)
    in_weight = noise(arg_keys[2], (D, COLS), D ** -0.5, 0.125, ((0, 128),))
    conv_weight = jnp.clip(jax.random.uniform(arg_keys[3], (CONV, INNER + 2 * STATE), jnp.float32, -0.6, 0.6), -0.6, 0.6)
    conv_bias = noise(arg_keys[4], (INNER + 2 * STATE,), 0.5, 3.0, (), jnp.float32)
    dt_bias = jnp.clip(jax.random.uniform(arg_keys[5], (HEADS,), jnp.float32, -4.0, 0.0), -4.0, 0.0)
    decay_rate = draw_decay_rate(jax.random.fold_in(arg_keys[9], 71), 0)
    skip_gain = jnp.clip(1.0 + 0.18 * jax.random.normal(arg_keys[7], (HEADS,), jnp.float32), 0.1, 1.9)
    norm_gain = jnp.clip(1.0 + 0.18 * jax.random.normal(arg_keys[8], (INNER,), jnp.float32), 0.1, 1.9)
    return dict(tokens=tokens, bounds=bounds, in_weight=in_weight, conv_weight=conv_weight, conv_bias=conv_bias, dt_bias=dt_bias, decay_rate=decay_rate, skip_gain=skip_gain, norm_gain=norm_gain)


def block_terms(head_input, input_map, output_map, step_size, decay_rate):
    log_decay = -(step_size * decay_rate[None, :]).T
    cumulative = jnp.cumsum(log_decay, axis=1)
    pairwise = cumulative[:, :, None] - cumulative[:, None, :]
    length = cumulative.shape[1]
    causal = jnp.arange(length)[:, None] >= jnp.arange(length)[None, :]
    pair_decay = jnp.exp(jnp.where(causal[None], pairwise, -jnp.inf))
    scores = jnp.dot(output_map, input_map.T, preferred_element_type=jnp.float32)
    mixing = scores[None] * pair_decay * step_size.T[:, None, :]
    inner_out = jnp.einsum('hij,jhp->ihp', mixing, head_input, precision=lax.Precision.HIGH)
    to_end = jnp.exp(cumulative[:, -1:] - cumulative) * step_size.T
    local_state = jnp.einsum('hj,jhp,jn->hpn', to_end, head_input, input_map.astype(jnp.float32), precision=lax.Precision.HIGH)
    return (inner_out, cumulative, local_state)

def carried(output_map, cumulative, state):
    reach = jnp.einsum('in,hpn->ihp', output_map.astype(jnp.float32), state, precision=lax.Precision.HIGH)
    return jnp.exp(cumulative).T[:, :, None] * reach

def one_sequence(tokens, bounds, in_weight, conv_weight, conv_bias, dt_bias, decay_rate, skip_gain, norm_gain):
    starts = bounds[:, 0]
    ends = bounds[:, 1]
    blocks = jnp.arange(TOTAL_BLOCKS).astype(jnp.int32)
    owner = lax.optimization_barrier(jnp.sum((ends[None, :] <= blocks[:, None]).astype(jnp.int32), axis=1)).astype(jnp.int32)
    slot_row = (owner * SLOT_BLOCKS + blocks - starts[owner]).astype(jnp.int32)
    grouped = tokens.reshape(N_SEQ * SLOT_BLOCKS, BLOCK, D)
    live = grouped[slot_row].reshape(SEQ_LEN, D)
    projected = jnp.dot(live, in_weight, preferred_element_type=jnp.float32).astype(jnp.bfloat16)
    gate = projected[:, :INNER].astype(jnp.float32)
    mixed_in = projected[:, INNER:2 * INNER + 2 * STATE]
    raw_step = projected[:, 2 * INNER + 2 * STATE:].astype(jnp.float32)
    padded = jnp.concatenate([jnp.zeros((CONV - 1, mixed_in.shape[1]), jnp.bfloat16), mixed_in], axis=0)
    convolved = jnp.zeros((SEQ_LEN, mixed_in.shape[1]), jnp.float32) + conv_bias[None, :]
    for offset in range(CONV):
        convolved = convolved + conv_weight[offset][None, :] * padded[offset:offset + SEQ_LEN].astype(jnp.float32)
    conv_out = jax.nn.silu(convolved).astype(jnp.bfloat16)
    head_input = conv_out[:, :INNER].astype(jnp.float32).reshape(TOTAL_BLOCKS, BLOCK, HEADS, HEAD_DIM)
    input_map = conv_out[:, INNER:INNER + STATE].reshape(TOTAL_BLOCKS, BLOCK, STATE)
    output_map = conv_out[:, INNER + STATE:].reshape(TOTAL_BLOCKS, BLOCK, STATE)
    step_size = jax.nn.softplus(raw_step + dt_bias[None, :]).reshape(TOTAL_BLOCKS, BLOCK, HEADS)

    def advance(state, pieces):
        in_values, in_map, out_map, in_step = pieces
        inner_out, cumulative, local_state = block_terms(in_values, in_map, out_map, in_step, decay_rate)
        result = inner_out + carried(out_map, cumulative, state) + skip_gain[None, :, None] * in_values
        state = jnp.exp(cumulative[:, -1])[:, None, None] * state + local_state
        return (state, result)
    initial = jnp.zeros((HEADS, HEAD_DIM, STATE), jnp.float32)
    final_state, outputs = lax.scan(advance, initial, (head_input, input_map, output_map, step_size))
    scanned = outputs.reshape(SEQ_LEN, INNER)
    gated = scanned * jax.nn.silu(gate)
    normed = gated * lax.rsqrt(lax.optimization_barrier(jnp.mean(gated * gated, axis=1, keepdims=True)) + 1e-05) * norm_gain[None, :]
    placed = jnp.zeros((N_SEQ * SLOT_BLOCKS, BLOCK, INNER), jnp.bfloat16)
    placed = placed.at[slot_row].set(normed.astype(jnp.bfloat16).reshape(TOTAL_BLOCKS, BLOCK, INNER))
    return placed.reshape(N_SEQ * SLOTS, INNER)

def reference(tokens, bounds, in_weight, conv_weight, conv_bias, dt_bias, decay_rate, skip_gain, norm_gain):
    results = [one_sequence(tokens[index], bounds[index], in_weight, conv_weight, conv_bias, dt_bias, decay_rate, skip_gain, norm_gain) for index in range(SEQS)]
    return jnp.stack(results)
```

```python
import jax
import jax.numpy as jnp
from jax import lax
from jax.experimental import pallas as pl
from jax.experimental.pallas import tpu as pltpu
from jax.sharding import Mesh
from jax.sharding import PartitionSpec as P

BLOCK = 256
EDGE = 8
SEQ_FSDP = ("seq_0", "seq_1", "seq_2", "fsdp")
SEQ = ("seq_0", "seq_1", "seq_2")
F32 = jnp.float32
BF16 = jnp.bfloat16


def passed_along(value, axis, steps):
    count = lax.axis_size(axis)
    leading, last = (max(0, -steps), min(count, count - steps))
    return lax.ppermute(value, axis, [(source, source + steps) for source in range(leading, last)])


def swapped(value):
    return lax.ppermute(value, "fsdp", [(0, 1), (1, 0)])


def block_terms(head_input, input_map, output_map, step_size, decay_rate):
    log_decay = -(step_size * decay_rate[None, :]).T
    cumulative = jnp.cumsum(log_decay, axis=1)
    pairwise = cumulative[:, :, None] - cumulative[:, None, :]
    length = cumulative.shape[1]
    causal = jnp.arange(length)[:, None] >= jnp.arange(length)[None, :]
    pair_decay = jnp.exp(jnp.where(causal[None], pairwise, -jnp.inf))
    scores = jnp.dot(output_map, input_map.T, preferred_element_type=jnp.float32)
    mixing = scores[None] * pair_decay * step_size.T[:, None, :]
    inner_out = jnp.einsum("hij,jhp->ihp", mixing, head_input, precision=lax.Precision.HIGH)
    to_end = jnp.exp(cumulative[:, -1:] - cumulative) * step_size.T
    local_state = jnp.einsum(
        "hj,jhp,jn->hpn",
        to_end,
        head_input,
        input_map.astype(jnp.float32),
        precision=lax.Precision.HIGH,
    )
    return (inner_out, cumulative, local_state)


def carried(output_map, cumulative, state):
    reach = jnp.einsum(
        "in,hpn->ihp", output_map.astype(jnp.float32), state, precision=lax.Precision.HIGH
    )
    return jnp.exp(cumulative).T[:, :, None] * reach


def prefix_kernel(count, rows, got_ref, out_ref):
    decays = jnp.exp(got_ref[:, rows, :]).T
    state = jnp.zeros((rows, got_ref.shape[2]), F32)
    for source in range(count):
        out_ref[source] = state
        if source < count - 1:
            factor = jnp.broadcast_to(decays[:rows, source : source + 1], state.shape)
            state = state * factor + got_ref[source, :rows, :]


def incoming_state(log_total, summary):
    heads, head_dim, width = summary.shape
    count = lax.axis_size(SEQ)
    rows = heads * head_dim // count
    per_row = jnp.repeat(log_total, head_dim).reshape(count, rows)
    parts = jnp.pad(per_row[:, None, :], ((0, 0), (0, 7), (0, width - rows)))
    payload = jnp.concatenate([summary.reshape(count, rows, width), parts], axis=1)
    got = lax.all_to_all(payload, SEQ, 0, 0, tiled=True)
    before = pl.pallas_call(
        lambda got_ref, out_ref: prefix_kernel(count, rows, got_ref, out_ref),
        out_shape=jax.ShapeDtypeStruct((count, rows, width), F32),
        cost_estimate=pl.CostEstimate(flops=8_000_000, bytes_accessed=1_500_000, transcendentals=0),
        name="prefix",
    )(got)
    back = lax.all_to_all(before, SEQ, 0, 0, tiled=True)
    return back.reshape(heads, head_dim, width)


def local(
    tokens, bounds, in_weight, conv_weight, conv_bias, dt_bias, decay_rate, skip_gain, norm_gain
):
    slots = tokens.shape[1]
    inner = norm_gain.shape[0]
    state_width = (conv_bias.shape[0] - inner) // 2
    heads = decay_rate.shape[0]
    head_dim = inner // heads
    kernel = conv_weight.shape[0]
    capacity = slots // BLOCK
    half = inner // 2
    core = lax.axis_index("fsdp")
    shard_blocks = bounds[0, 0, 1] - bounds[0, 0, 0]
    own_rows = tokens[0]

    def columns(which):
        early = jnp.concatenate(
            [
                lax.dynamic_slice_in_dim(in_weight, inner + half * which, half, 1),
                lax.dynamic_slice_in_dim(in_weight, 2 * inner + state_width * which, state_width, 1),
                in_weight[:, 2 * inner + 2 * state_width :],
            ],
            axis=1,
        )
        return early, lax.dynamic_slice_in_dim(in_weight, half * which, half, 1)

    mine, mine_gate = columns(core)
    other, other_gate = columns(1 - core)

    def paired(kept, sent):
        received = swapped(sent)
        return jnp.where(
            core == 0,
            jnp.concatenate([kept, received], axis=0),
            jnp.concatenate([received, kept], axis=0),
        )

    early_weight = lax.all_gather(paired(mine, other), SEQ, axis=0, tiled=True)
    gate_weight = lax.all_gather(paired(mine_gate, other_gate), SEQ, axis=0, tiled=True)
    edge = lax.dynamic_slice_in_dim(own_rows, shard_blocks * BLOCK - EDGE, EDGE, 0)
    own_all = jnp.concatenate([own_rows, passed_along(edge, SEQ, 1)], axis=0)
    other_all = swapped(own_all)

    def projected(rows, weight):
        return jnp.dot(rows, weight, preferred_element_type=F32).astype(BF16)

    got = swapped(projected(other_all, early_weight)[:, : half + state_width])
    kept = projected(own_all, early_weight)
    raw_step = kept[:slots, half + state_width :].astype(F32)
    low = jnp.where(core == 0, kept[:, : half + state_width], got)
    high = jnp.where(core == 0, got, kept[:, : half + state_width])
    mixed = jnp.concatenate([low[:, :half], high[:, :half], low[:, half:], high[:, half:]], axis=1)
    extended = jnp.concatenate([mixed[slots + EDGE - kernel + 1 :], mixed[:slots]], axis=0)
    convolved = jnp.zeros((slots, mixed.shape[1]), F32) + conv_bias[None, :]
    for offset in range(kernel):
        convolved = convolved + conv_weight[offset][None, :] * extended[
            offset : offset + slots
        ].astype(F32)
    conv_out = jax.nn.silu(convolved).astype(BF16)
    live_mask = jnp.arange(slots)[:, None] < shard_blocks * BLOCK
    step_size = jnp.where(live_mask, jax.nn.softplus(raw_step + dt_bias[None, :]), 0.0)
    pieces = []
    log_total = jnp.zeros((heads,), F32)
    summary_state = jnp.zeros((heads, head_dim, state_width), F32)
    for place in range(capacity):
        lower = place * BLOCK
        upper = lower + BLOCK
        in_values = conv_out[lower:upper, :inner].astype(F32).reshape(BLOCK, heads, head_dim)
        in_map = conv_out[lower:upper, inner : inner + state_width]
        out_map = conv_out[lower:upper, inner + state_width :]
        inner_out, cumulative, local_state = block_terms(
            in_values, in_map, out_map, step_size[lower:upper], decay_rate
        )
        block_decay = jnp.exp(cumulative[:, -1])
        summary_state = block_decay[:, None, None] * summary_state + local_state
        log_total = log_total + cumulative[:, -1]
        pieces.append((in_values, out_map, inner_out, cumulative, local_state, block_decay))
    state = incoming_state(log_total, summary_state)
    gate_weight, _ = lax.optimization_barrier((gate_weight, summary_state))

    got_gate = swapped(projected(other_all[:slots], gate_weight))
    kept_gate = projected(own_rows, gate_weight)
    gate = jnp.concatenate(
        [jnp.where(core == 0, kept_gate, got_gate), jnp.where(core == 0, got_gate, kept_gate)],
        axis=1,
    ).astype(F32)
    results = []
    for in_values, out_map, inner_out, cumulative, local_state, block_decay in pieces:
        result = (
            inner_out + carried(out_map, cumulative, state) + skip_gain[None, :, None] * in_values
        )
        results.append(result.reshape(BLOCK, inner))
        state = block_decay[:, None, None] * state + local_state
    scanned = jnp.concatenate(results, axis=0)
    gated = scanned * jax.nn.silu(gate)
    normed = (
        gated
        * lax.rsqrt(jnp.mean(gated * gated, axis=1, keepdims=True) + 1e-05)
        * norm_gain[None, :]
    )
    layer_out = jnp.where(live_mask, normed, 0.0).astype(BF16)
    return layer_out[None]


def solution(mesh):
    split = Mesh(
        mesh.devices.reshape(4, 4, 4, mesh.shape["fsdp"]), ("seq_0", "seq_1", "seq_2", "fsdp")
    )
    return jax.shard_map(
        local,
        mesh=split,
        in_specs=(
            P("fsdp", SEQ, None),
            P("fsdp", SEQ, None),
            P(SEQ_FSDP, None),
            P(),
            P(),
            P(),
            P(),
            P(),
            P(),
        ),
        out_specs=P("fsdp", SEQ, None),
        check_vma=False,
    )
```

```python
import functools

import jax
import jax.numpy as jnp
from jax import lax
from jax.experimental import pallas as pl
from jax.experimental.pallas import tpu as pltpu
from jax.sharding import Mesh
from jax.sharding import PartitionSpec as P

BLOCK = 256
EDGE = 8
SEQ_FSDP = ("seq_0", "seq_1", "seq_2", "fsdp")
SEQ = ("seq_0", "seq_1", "seq_2")
F32 = jnp.float32
BF16 = jnp.bfloat16


def passed_along(value, axis, steps):
    count = lax.axis_size(axis)
    leading, last = (max(0, -steps), min(count, count - steps))
    return lax.ppermute(value, axis, [(source, source + steps) for source in range(leading, last)])


def swapped(value):
    return lax.ppermute(value, "fsdp", [(0, 1), (1, 0)])


def split_dot(left, right, dims):
    high = right.astype(BF16)
    low = (right - high.astype(F32)).astype(BF16)
    dot = lambda part: lax.dot_general(left, part, (dims, ((), ())), preferred_element_type=F32)
    return dot(high) + dot(low)


def spread(table, lanes):
    index = jnp.broadcast_to(lanes, table.shape)
    return jnp.take_along_axis(table, index, axis=1)


def lane_ids(shape):
    return lax.broadcasted_iota(jnp.int32, shape, 1)


def front_kernel(
    heads, head_dim, chunk_rows,
    scalars, kept_ref, got_ref, kept_map_ref, got_map_ref, raw_ref, conv_ref, map_conv_ref, head_ref,
    x_ref, maps_ref, cum_ref, step_ref, pay_ref,
    ext, factor, turned, high, low,
):
    group = pl.program_id(0)
    groups = pl.num_programs(0)
    slots, width = x_ref.shape
    chunk = 128

    def fill(ref):
        ext[:EDGE, :] = ref[slots:, :].astype(F32)
        ext[EDGE:, :] = ref[:slots, :].astype(F32)

    def convolve(taps, start):
        first = EDGE - 3 + start
        total = taps[4:5, :] + taps[0:1, :] * ext[first : first + chunk, :]
        for offset in range(1, 4):
            total = total + taps[offset : offset + 1, :] * ext[first + offset : first + offset + chunk, :]
        return (total * jax.nn.sigmoid(total)).astype(BF16)

    @pl.when(group == 0)
    def _():
        core, live = scalars[0], scalars[1]
        for which in range(2):
            taps = map_conv_ref[:, which * width : (which + 1) * width]

            @pl.when(core == which)
            def _():
                fill(kept_map_ref)

            @pl.when(core != which)
            def _():
                fill(got_map_ref)

            for start in range(0, slots, chunk):
                value = convolve(taps, start)
                maps_ref[start : start + chunk, which * width : (which + 1) * width] = value
                if which == 0:
                    turned[:, start : start + chunk] = value.astype(F32).T.astype(BF16)
        lanes = lane_ids((slots, width))
        rows = lax.broadcasted_iota(jnp.int32, (slots, width), 0)
        shifted = raw_ref[:slots, :].astype(F32) + head_ref[0:1, :]
        step = jnp.maximum(shifted, 0.0) + jnp.log1p(jnp.exp(-jnp.abs(shifted)))
        step = jnp.where((lanes < heads) & (rows < live), step, 0.0)
        step_ref[...] = step
        log_decay = -(step * head_ref[1:2, :])
        triangle = (
            lax.broadcasted_iota(jnp.int32, (BLOCK, BLOCK), 0) >= lane_ids((BLOCK, BLOCK))
        ).astype(F32)
        before = jnp.zeros((1, width), F32)
        for lower in range(0, slots, BLOCK):
            cum = jnp.dot(
                triangle,
                log_decay[lower : lower + BLOCK],
                precision=lax.Precision.HIGHEST,
                preferred_element_type=F32,
            )
            cum_ref[lower : lower + BLOCK, :] = cum
            factor[lower : lower + BLOCK, :] = cum + before
            before = before + cum[BLOCK - 1 :, :]
        factor[...] = jnp.exp(before - factor[...]) * step
        pay_ref[:, chunk_rows:, :] = jnp.broadcast_to(
            before[None], (pay_ref.shape[0], pay_ref.shape[1] - chunk_rows, width)
        )

    @pl.when(group < groups // 2)
    def _():
        fill(kept_ref)

    @pl.when(group >= groups // 2)
    def _():
        fill(got_ref)

    lanes = group * (width // head_dim) + lane_ids((1, width)) // head_dim
    taps = conv_ref[...]
    for start in range(0, slots, chunk):
        value = convolve(taps, start)
        x_ref[start : start + chunk, :] = value
        weighted = value.astype(F32) * spread(factor[start : start + chunk, :], lanes)
        top = weighted.astype(BF16)
        high[start : start + chunk, :] = top
        low[start : start + chunk, :] = (weighted - top.astype(F32)).astype(BF16)
    state = jnp.dot(turned[...], high[...], preferred_element_type=F32) + jnp.dot(
        turned[...], low[...], preferred_element_type=F32
    )
    state = state.T
    pieces = chunk_rows // 8
    for k in range(width // 8):
        place = group * (width // 8) + k
        row = pl.multiple_of(lax.rem(place, pieces) * 8, 8)
        pay_ref[lax.div(place, pieces), pl.ds(row, 8), :] = state[8 * k : 8 * k + 8, :]


def inner_kernel(
    head_dim,
    x_ref, maps_ref, cum_ref, step_ref, skip_ref, y_ref,
    run, scores, turned, across,
):
    block, group = pl.program_id(0), pl.program_id(1)
    rows, width = x_ref.shape
    part = rows // 2

    @pl.when(group == 0)
    def _():
        b = maps_ref[:, :width]
        c = maps_ref[:, width:]
        scores[...] = lax.dot_general(c, b, (((1,), (1,)), ((), ())), preferred_element_type=F32)
        turned[...] = b.astype(F32).T.astype(BF16)
        across[...] = (cum_ref[...] - jnp.log(step_ref[...])).T

    @pl.when(block == 0)
    def _():
        run[group] = jnp.zeros(run.shape[1:], F32)

    first_head = group * (width // head_dim)
    lane = lane_ids((1, width))
    cum = cum_ref[...]
    by_head = [spread(cum, jnp.zeros((1, width), jnp.int32) + first_head + e) for e in range(2)]
    low_lanes = lane_ids((rows, width)) < head_dim
    cum_x = jnp.where(low_lanes, by_head[0], by_head[1])
    step_x = spread(step_ref[...], first_head + lane // head_dim)
    x = x_ref[...]
    causal = lax.broadcasted_iota(jnp.int32, (part, part), 0) >= lane_ids((part, part))
    outs = []
    for e in range(2):
        row = across[pl.ds(first_head + e, 1), :]
        column = by_head[e]

        def mixing(i, j):
            exponent = column[i * part : (i + 1) * part, :] - row[:, j * part : (j + 1) * part]
            if i == j:
                exponent = jnp.where(causal, exponent, -jnp.inf)
            value = jnp.exp(exponent) * scores[i * part : (i + 1) * part, j * part : (j + 1) * part]
            top = value.astype(BF16)
            return top, (value - top.astype(F32)).astype(BF16)

        m00, m10, m11 = mixing(0, 0), mixing(1, 0), mixing(1, 1)
        dot = lambda m, j: jnp.dot(m, x[j * part : (j + 1) * part], preferred_element_type=F32)
        outs.append(
            jnp.concatenate(
                [
                    dot(m00[0], 0) + dot(m00[1], 0),
                    (dot(m10[0], 0) + dot(m10[1], 0)) + (dot(m11[0], 1) + dot(m11[1], 1)),
                ],
                axis=0,
            )
        )
    x32 = x.astype(F32)
    state = run[group]
    reach = split_dot(maps_ref[:, width:], state, ((1,), (0,)))
    y_ref[...] = (
        jnp.where(low_lanes, outs[0], outs[1]) + jnp.exp(cum_x) * reach + skip_ref[0:1, :] * x32
    )
    end = cum_x[rows - 1 :, :]
    weighted = x32 * (jnp.exp(end - cum_x) * step_x)
    run[group] = jnp.exp(end) * state + split_dot(turned[...], weighted, ((1,), (0,)))


def finish_kernel(
    head_dim,
    scalars, kept_ref, got_ref, y_ref, c_ref, cum_ref, state_ref, gain_ref, out_ref,
    high, low, before, gated,
):
    block = pl.program_id(0)
    rows, inner = y_ref.shape
    width = c_ref.shape[1]
    groups = inner // width

    @pl.when(block == 0)
    def _():
        state = state_ref[...]
        top = state.astype(BF16)
        high[...] = top
        low[...] = (state - top.astype(F32)).astype(BF16)
        before[...] = jnp.zeros(before.shape, F32)

    cum = cum_ref[...] + before[0:1, :]
    before[...] = jnp.broadcast_to(cum[rows - 1 :, :], before.shape)
    reached = jnp.exp(cum)
    c = c_ref[...]
    lane = lane_ids((1, width))

    def half(gate_ref, first):
        def body(k, total):
            group = first + k
            at = pl.ds(pl.multiple_of(group * width, width), width)
            dot = lambda part: lax.dot_general(
                c, part[at, :], (((1,), (1,)), ((), ())), preferred_element_type=F32
            )
            carried = spread(reached, group * (width // head_dim) + lane // head_dim) * (
                dot(high) + dot(low)
            )
            gate = gate_ref[:, pl.ds(pl.multiple_of(k * width, width), width)].astype(F32)
            value = (y_ref[:, at] + carried) * (gate * jax.nn.sigmoid(gate))
            gated[:, at] = value
            return total + value * value

        return body

    total = jnp.zeros((rows, width), F32)
    total = lax.fori_loop(0, groups // 2, half(kept_ref, 0), total)
    total = lax.fori_loop(0, groups // 2, half(got_ref, groups // 2), total)
    scale = lax.rsqrt(jnp.sum(total, axis=1, keepdims=True) / inner + 1e-05)
    live = lax.broadcasted_iota(jnp.int32, (rows, 1), 0) + block * rows < scalars[1]
    shift = scalars[0] * (groups // 2)

    def write(group, _):
        at = pl.ds(pl.multiple_of(group * width, width), width)
        target = lax.rem(group + shift, groups)
        value = gated[:, at] * scale * gain_ref[0:1, at]
        out_ref[:, pl.ds(pl.multiple_of(target * width, width), width)] = jnp.where(
            live, value, 0.0
        ).astype(BF16)
        return _

    lax.fori_loop(0, groups, write, 0)


def prefix_kernel(count, rows, head_dim, place_ref, got_ref, out_ref, turned):
    first = lax.div(place_ref[0] * rows, head_dim)
    edge = (first + 1) * head_dim - place_ref[0] * rows
    turned[...] = got_ref[:, rows, :].T
    shape = (rows, count)
    decays = jnp.exp(
        jnp.where(
            lax.broadcasted_iota(jnp.int32, shape, 0) < edge,
            jnp.broadcast_to(turned[pl.ds(first, 1), :], shape),
            jnp.broadcast_to(turned[pl.ds(first + 1, 1), :], shape),
        )
    )
    state = jnp.zeros((rows, got_ref.shape[2]), F32)
    for source in range(count):
        out_ref[source] = state
        if source < count - 1:
            factor = jnp.broadcast_to(decays[:, source : source + 1], state.shape)
            state = state * factor + got_ref[source, :rows, :]


def local(
    tokens, bounds, in_weight, conv_weight, conv_bias, dt_bias, decay_rate, skip_gain, norm_gain
):
    slots = tokens.shape[1]
    inner = norm_gain.shape[0]
    state_width = (conv_bias.shape[0] - inner) // 2
    heads = decay_rate.shape[0]
    head_dim = inner // heads
    kernel = conv_weight.shape[0]
    capacity = slots // BLOCK
    half = inner // 2
    core = lax.axis_index("fsdp")
    shard_blocks = bounds[0, 0, 1] - bounds[0, 0, 0]
    own_rows = tokens[0]

    def turned_by_core(value, which, axis):
        middle = value.shape[axis] // 2
        first = lax.slice_in_dim(value, 0, middle, axis=axis)
        second = lax.slice_in_dim(value, middle, 2 * middle, axis=axis)
        return jnp.where(
            which == 0,
            jnp.concatenate([first, second], axis),
            jnp.concatenate([second, first], axis),
        )

    def columns(which):
        early = jnp.concatenate(
            [
                lax.dynamic_slice_in_dim(in_weight, inner + half * which, half, 1),
                lax.dynamic_slice_in_dim(in_weight, 2 * inner + state_width * which, state_width, 1),
                turned_by_core(in_weight[:, 2 * inner + 2 * state_width :], which, 1),
            ],
            axis=1,
        )
        return early, lax.dynamic_slice_in_dim(in_weight, half * which, half, 1)

    mine, mine_gate = columns(core)
    other, other_gate = columns(1 - core)

    def paired(kept, sent):
        received = swapped(sent)
        return jnp.where(
            core == 0,
            jnp.concatenate([kept, received], axis=0),
            jnp.concatenate([received, kept], axis=0),
        )

    early_weight = lax.all_gather(paired(mine, other), SEQ, axis=0, tiled=True)
    gate_weight = lax.all_gather(paired(mine_gate, other_gate), SEQ, axis=0, tiled=True)
    edge = lax.dynamic_slice_in_dim(own_rows, shard_blocks * BLOCK - EDGE, EDGE, 0)
    own_all = jnp.concatenate([own_rows, passed_along(edge, SEQ, 1)], axis=0)
    other_all = swapped(own_all)

    def projected(rows, weight):
        return jnp.dot(rows, weight, preferred_element_type=F32).astype(BF16)

    groups = inner // state_width
    taps = jnp.pad(
        jnp.concatenate([conv_weight, conv_bias[None, :]], axis=0), ((0, 8 - kernel - 1), (0, 0))
    )
    map_taps = taps[:, inner:]
    taps = turned_by_core(taps[:, :inner], core, 1)
    head_rows = turned_by_core(jnp.stack([dt_bias, decay_rate]), core, 1)
    head_rows = jnp.pad(head_rows, ((0, 6), (0, state_width - heads)))
    skip = jnp.broadcast_to(
        jnp.repeat(turned_by_core(skip_gain, core, 0), head_dim)[None, :], (8, inner)
    )
    gain = jnp.broadcast_to(turned_by_core(norm_gain, core, 0)[None, :], (8, inner))
    scalars = jnp.stack([core.astype(jnp.int32), shard_blocks * BLOCK])
    count = lax.axis_size(SEQ)
    chunk_rows = inner // count

    got = swapped(projected(other_all, early_weight)[:, : half + state_width])
    kept = projected(own_all, early_weight)
    total_rows = slots + EDGE
    last = groups // 2
    tile = lambda rows, index: pl.BlockSpec((rows, state_width), index)
    whole = lambda shape: pl.BlockSpec(shape, lambda *_: (0,) * len(shape))
    xs, maps, cum, step, payload = pl.pallas_call(
        functools.partial(front_kernel, heads, head_dim, chunk_rows),
        grid=(groups,),
        in_specs=[
            pl.BlockSpec(memory_space=pltpu.SMEM),
            tile(total_rows, lambda g: (0, jnp.minimum(g, last - 1))),
            tile(total_rows, lambda g: (0, jnp.maximum(g - last, 0))),
            tile(total_rows, lambda g: (0, last)),
            tile(total_rows, lambda g: (0, last)),
            tile(total_rows, lambda g: (0, last + 1)),
            tile(8, lambda g: (0, g)),
            whole((8, 2 * state_width)),
            whole((8, state_width)),
        ],
        out_specs=[
            tile(slots, lambda g: (0, g)),
            whole((slots, 2 * state_width)),
            whole((slots, state_width)),
            whole((slots, state_width)),
            whole((count, chunk_rows + 8, state_width)),
        ],
        out_shape=[
            jax.ShapeDtypeStruct((slots, inner), BF16),
            jax.ShapeDtypeStruct((slots, 2 * state_width), BF16),
            jax.ShapeDtypeStruct((slots, state_width), F32),
            jax.ShapeDtypeStruct((slots, state_width), F32),
            jax.ShapeDtypeStruct((count, chunk_rows + 8, state_width), F32),
        ],
        scratch_shapes=[
            pltpu.VMEM((total_rows, state_width), F32),
            pltpu.VMEM((slots, state_width), F32),
            pltpu.VMEM((state_width, slots), BF16),
            pltpu.VMEM((slots, state_width), BF16),
            pltpu.VMEM((slots, state_width), BF16),
        ],
        cost_estimate=pl.CostEstimate(flops=4_000_000_000, bytes_accessed=12_000_000, transcendentals=4_000_000),
        name="front",
    )(scalars, kept, got, kept, got, kept, taps, map_taps, head_rows)

    received = lax.all_to_all(payload, SEQ, 0, 0, tiled=True)
    block_tile = lambda columns, index: pl.BlockSpec((BLOCK, columns), index)
    y = pl.pallas_call(
        functools.partial(inner_kernel, head_dim),
        grid=(capacity, groups),
        in_specs=[
            block_tile(state_width, lambda q, g: (q, g)),
            block_tile(2 * state_width, lambda q, g: (q, 0)),
            block_tile(state_width, lambda q, g: (q, 0)),
            block_tile(state_width, lambda q, g: (q, 0)),
            pl.BlockSpec((8, state_width), lambda q, g: (0, g)),
        ],
        out_specs=block_tile(state_width, lambda q, g: (q, g)),
        out_shape=jax.ShapeDtypeStruct((slots, inner), F32),
        scratch_shapes=[
            pltpu.VMEM((groups, state_width, state_width), F32),
            pltpu.VMEM((BLOCK, BLOCK), F32),
            pltpu.VMEM((state_width, BLOCK), BF16),
            pltpu.VMEM((state_width, BLOCK), F32),
        ],
        cost_estimate=pl.CostEstimate(flops=20_000_000_000, bytes_accessed=14_000_000, transcendentals=12_000_000),
        name="inner",
    )(xs, maps, cum, step, skip)

    gate_weight, _ = lax.optimization_barrier((gate_weight, y))
    got_gate = swapped(projected(other_all[:slots], gate_weight))
    kept_gate = projected(own_rows, gate_weight)

    before = pl.pallas_call(
        functools.partial(prefix_kernel, count, chunk_rows, head_dim),
        in_specs=[pl.BlockSpec(memory_space=pltpu.SMEM), pl.BlockSpec(memory_space=pltpu.VMEM)],
        out_specs=pl.BlockSpec(memory_space=pltpu.VMEM),
        out_shape=jax.ShapeDtypeStruct((count, chunk_rows, state_width), F32),
        scratch_shapes=[pltpu.VMEM((state_width, count), F32)],
        cost_estimate=pl.CostEstimate(flops=2_000_000_000, bytes_accessed=3_000_000, transcendentals=0),
        name="prefix",
    )(lax.axis_index(SEQ).astype(jnp.int32)[None], received)
    state = lax.all_to_all(before, SEQ, 0, 0, tiled=True).reshape(inner, state_width)

    layer_out = pl.pallas_call(
        functools.partial(finish_kernel, head_dim),
        grid=(capacity,),
        in_specs=[
            pl.BlockSpec(memory_space=pltpu.SMEM),
            block_tile(half, lambda q: (q, 0)),
            block_tile(half, lambda q: (q, 0)),
            block_tile(inner, lambda q: (q, 0)),
            block_tile(state_width, lambda q: (q, 1)),
            block_tile(state_width, lambda q: (q, 0)),
            whole((inner, state_width)),
            whole((8, inner)),
        ],
        out_specs=block_tile(inner, lambda q: (q, 0)),
        out_shape=jax.ShapeDtypeStruct((slots, inner), BF16),
        scratch_shapes=[
            pltpu.VMEM((inner, state_width), BF16),
            pltpu.VMEM((inner, state_width), BF16),
            pltpu.VMEM((8, state_width), F32),
            pltpu.VMEM((BLOCK, inner), F32),
        ],
        cost_estimate=pl.CostEstimate(flops=4_000_000_000, bytes_accessed=18_000_000, transcendentals=4_000_000),
        name="finish",
    )(scalars, kept_gate, got_gate, y, maps, cum, state, gain)
    return layer_out[None]


def solution(mesh):
    split = Mesh(
        mesh.devices.reshape(4, 4, 4, mesh.shape["fsdp"]), ("seq_0", "seq_1", "seq_2", "fsdp")
    )
    return jax.shard_map(
        local,
        mesh=split,
        in_specs=(
            P("fsdp", SEQ, None),
            P("fsdp", SEQ, None),
            P(SEQ_FSDP, None),
            P(),
            P(),
            P(),
            P(),
            P(),
            P(),
        ),
        out_specs=P("fsdp", SEQ, None),
        check_vma=False,
    )
```

```python
import functools

import jax
import jax.numpy as jnp
from jax import lax
from jax.experimental import pallas as pl
from jax.experimental.pallas import tpu as pltpu
from jax.sharding import Mesh
from jax.sharding import PartitionSpec as P


BLOCK = 256
EDGE = 8
SEQ_FSDP = ("seq_0", "seq_1", "seq_2", "fsdp")
SEQ = ("seq_0", "seq_1", "seq_2")
F32 = jnp.float32
BF16 = jnp.bfloat16


def passed_along(value, axis, steps):
    count = lax.axis_size(axis)
    leading, last = (max(0, -steps), min(count, count - steps))
    return lax.ppermute(value, axis, [(source, source + steps) for source in range(leading, last)])


def swapped(value):
    return lax.ppermute(value, "fsdp", [(0, 1), (1, 0)])


def pack_kernel(inner, width, core_ref, weight_ref, kept_ref, sent_ref):
    half = inner // 2
    for which, target in ((core_ref[0], kept_ref), (1 - core_ref[0], sent_ref)):
        columns = lambda start, count: weight_ref[:, pl.ds(pl.multiple_of(start, 128), count)]
        target[:, :half] = columns(inner + half * which, half)
        target[:, half : half + width] = columns(2 * inner + width * which, width)
        steps = weight_ref.shape[1] - 2 * inner - 2 * width
        target[:, half + width : half + width + steps] = columns(2 * inner + 2 * width, steps)
        target[:, half + 2 * width :] = columns(half * which, half)


def project_kernel(rows_ref, weight_ref, out_ref):
    out_ref[...] = jnp.dot(
        rows_ref[...], weight_ref[...], preferred_element_type=F32
    ).astype(BF16)


def project(rows, weight, first, count):
    tile = 256
    return pl.pallas_call(
        project_kernel,
        grid=(count // tile,),
        in_specs=[
            pl.BlockSpec(memory_space=pltpu.VMEM),
            pl.BlockSpec((weight.shape[0], tile), lambda j: (0, first // tile + j)),
        ],
        out_specs=pl.BlockSpec((rows.shape[0], tile), lambda j: (0, j)),
        out_shape=jax.ShapeDtypeStruct((rows.shape[0], count), BF16),
        cost_estimate=pl.CostEstimate(
            flops=2 * rows.shape[0] * weight.shape[0] * count, bytes_accessed=14_000_000, transcendentals=0
        ),
        name="project_gate",
    )(rows, weight)


def split_dot(left, right, dims):
    high = right.astype(BF16)
    low = (right - high.astype(F32)).astype(BF16)
    dot = lambda part: lax.dot_general(left, part, (dims, ((), ())), preferred_element_type=F32)
    return dot(high) + dot(low)


def spread(table, lanes):
    index = jnp.broadcast_to(lanes, table.shape)
    return jnp.take_along_axis(table, index, axis=1)


def padded_row(ref, width):
    row = ref[...]
    return jnp.concatenate([row, jnp.zeros((1, width - row.shape[1]), row.dtype)], axis=1)


def lane_ids(shape):
    return lax.broadcasted_iota(jnp.int32, shape, 1)


def front_kernel(
    heads, head_dim, chunk_rows,
    scalars, kept_ref, got_ref, kept_map_ref, got_map_ref, raw_ref, conv_ref, bias_ref, map_conv_ref, map_bias_ref, dt_ref, decay_ref,
    x_ref, maps_ref, cum_ref, step_ref, pay_ref,
    ext, factor, turned, high, low,
):
    part = pl.program_id(0)
    parts = pl.num_programs(0)
    slots, width = cum_ref.shape
    inside = x_ref.shape[1] // width
    chunk = 128

    def fill(ref, at, slot=0):
        ext[slot, :EDGE, :] = ref[slots:, at].astype(F32)
        ext[slot, EDGE:, :] = ref[:slots, at].astype(F32)

    def convolve(taps, bias, start, slot=0):
        first = EDGE - 3 + start
        total = bias + taps[0:1, :] * ext[slot, first : first + chunk, :]
        for offset in range(1, 4):
            total = total + taps[offset : offset + 1, :] * ext[slot, first + offset : first + offset + chunk, :]
        return (total * jax.nn.sigmoid(total)).astype(BF16)

    @pl.when(part == 0)
    def _():
        core, live = scalars[0], scalars[1]
        for which in range(2):
            taps = map_conv_ref[:, which * width : (which + 1) * width]
            bias = map_bias_ref[:, which * width : (which + 1) * width]

            @pl.when(core == which)
            def _():
                fill(kept_map_ref, pl.ds(0, width))

            @pl.when(core != which)
            def _():
                fill(got_map_ref, pl.ds(0, width))

            for start in range(0, slots, chunk):
                value = convolve(taps, bias, start)
                maps_ref[start : start + chunk, which * width : (which + 1) * width] = value
                if which == 0:
                    turned[:, start : start + chunk] = value.astype(F32).T.astype(BF16)
        lanes = lane_ids((slots, width))
        rows = lax.broadcasted_iota(jnp.int32, (slots, width), 0)
        turned_lanes = lane_ids((1, width)) + core * (heads // 2)
        turned_lanes = jnp.where(turned_lanes < heads, turned_lanes, turned_lanes - heads)
        turned_lanes = jnp.where(lane_ids((1, width)) < heads, turned_lanes, 0)
        row = lambda ref: spread(jnp.broadcast_to(padded_row(ref, width), (8, width)), turned_lanes)[0:1, :]
        shifted = spread(raw_ref[:slots, :].astype(F32), turned_lanes) + row(dt_ref)
        step = jnp.maximum(shifted, 0.0) + jnp.log1p(jnp.exp(-jnp.abs(shifted)))
        step = jnp.where((lanes < heads) & (rows < live), step, 0.0)
        step_ref[...] = step
        log_decay = -(step * jnp.where(lane_ids((1, width)) < heads, row(decay_ref), 0.0))
        triangle = (
            lax.broadcasted_iota(jnp.int32, (BLOCK, BLOCK), 0) >= lane_ids((BLOCK, BLOCK))
        ).astype(F32)
        before = jnp.zeros((1, width), F32)
        for lower in range(0, slots, BLOCK):
            cum = jnp.dot(
                triangle,
                log_decay[lower : lower + BLOCK],
                precision=lax.Precision.HIGHEST,
                preferred_element_type=F32,
            )
            cum_ref[lower : lower + BLOCK, :] = cum
            factor[lower : lower + BLOCK, :] = cum + before
            before = before + cum[BLOCK - 1 :, :]
        factor[...] = jnp.exp(before - factor[...]) * step
        pay_ref[:, chunk_rows:, :] = jnp.broadcast_to(
            before[None], (pay_ref.shape[0], pay_ref.shape[1] - chunk_rows, width)
        )

    @pl.when(part < parts // 2)
    def _():
        for k in range(inside):
            fill(kept_ref, pl.ds(k * width, width), k)

    @pl.when(part >= parts // 2)
    def _():
        for k in range(inside):
            fill(got_ref, pl.ds(k * width, width), k)

    for k in range(inside):
        group = part * inside + k
        at = pl.ds(k * width, width)
        odd = k % 2

        lanes = group * (width // head_dim) + lane_ids((1, width)) // head_dim
        taps, bias = conv_ref[:, at], bias_ref[:, at]
        for start in range(0, slots, chunk):
            value = convolve(taps, bias, start, k)
            x_ref[start : start + chunk, at] = value
            weighted = value.astype(F32) * spread(factor[start : start + chunk, :], lanes)
            top = weighted.astype(BF16)
            high[odd, start : start + chunk, :] = top
            low[odd, start : start + chunk, :] = (weighted - top.astype(F32)).astype(BF16)
        state = jnp.dot(turned[...], high[odd], preferred_element_type=F32) + jnp.dot(
            turned[...], low[odd], preferred_element_type=F32
        )
        state = state.T
        pieces = chunk_rows // 8
        for r in range(width // 8):
            place = group * (width // 8) + r
            row = pl.multiple_of(lax.rem(place, pieces) * 8, 8)
            pay_ref[lax.div(place, pieces), pl.ds(row, 8), :] = state[8 * r : 8 * r + 8, :]


def inner_kernel(
    head_dim, heads,
    scalars, x_ref, maps_ref, cum_ref, step_ref, skip_ref, y_ref,
    run, scores, turned, across,
):
    block = pl.program_id(0)
    rows, width = cum_ref.shape
    part = rows // 2
    b, c = maps_ref[:, :width], maps_ref[:, width:]
    scores[...] = lax.dot_general(c, b, (((1,), (1,)), ((), ())), preferred_element_type=F32)
    turned[...] = b.astype(F32).T.astype(BF16)
    across[...] = (cum_ref[...] - jnp.log(step_ref[...])).T

    @pl.when(block == 0)
    def _():
        run[...] = jnp.zeros(run.shape, F32)

    lane = lane_ids((1, width))
    low_lanes = lane_ids((rows, width)) < head_dim
    causal = lax.broadcasted_iota(jnp.int32, (part, part), 0) >= lane_ids((part, part))
    skips = jnp.broadcast_to(padded_row(skip_ref, width), (8, width))

    def each(group, carry):
        at = pl.ds(pl.multiple_of(group * width, width), width)
        first_head = group * (width // head_dim)
        cum = cum_ref[...]
        by_head = [spread(cum, jnp.zeros((1, width), jnp.int32) + first_head + e) for e in range(2)]
        cum_x = jnp.where(low_lanes, by_head[0], by_head[1])
        step_x = spread(step_ref[...], first_head + lane // head_dim)
        x = x_ref[:, at]
        outs = []
        for e in range(2):
            row = across[pl.ds(first_head + e, 1), :]
            column = by_head[e]

            def mixing(i, j):
                exponent = column[i * part : (i + 1) * part, :] - row[:, j * part : (j + 1) * part]
                if i == j:
                    exponent = jnp.where(causal, exponent, -jnp.inf)
                value = jnp.exp(exponent) * scores[i * part : (i + 1) * part, j * part : (j + 1) * part]
                top = value.astype(BF16)
                return top, (value - top.astype(F32)).astype(BF16)

            m00, m10, m11 = mixing(0, 0), mixing(1, 0), mixing(1, 1)
            dot = lambda m, j: jnp.dot(m, x[j * part : (j + 1) * part], preferred_element_type=F32)
            outs.append(
                jnp.concatenate(
                    [
                        dot(m00[0], 0) + dot(m00[1], 0),
                        (dot(m10[0], 0) + dot(m10[1], 0)) + (dot(m11[0], 1) + dot(m11[1], 1)),
                    ],
                    axis=0,
                )
            )
        x32 = x.astype(F32)
        turned_head = first_head + scalars[0] * (heads // 2)
        turned_head = jnp.where(turned_head < heads, turned_head, turned_head - heads)
        skip = spread(skips, turned_head + lane // head_dim)
        state = run[group]
        reach = split_dot(maps_ref[:, width:], state, ((1,), (0,)))
        y_ref[:, at] = (
            jnp.where(low_lanes, outs[0], outs[1]) + jnp.exp(cum_x) * reach + skip[0:1, :] * x32
        )
        end = cum_x[rows - 1 :, :]
        weighted = x32 * (jnp.exp(end - cum_x) * step_x)
        run[group] = jnp.exp(end) * state + split_dot(turned[...], weighted, ((1,), (0,)))
        return carry

    lax.fori_loop(0, run.shape[0], each, 0, unroll=4)


def finish_kernel(
    head_dim,
    scalars, kept_ref, got_ref, y_ref, c_ref, cum_ref, state_ref, gain_ref, out_ref,
    high, low, before, gated,
):
    block = pl.program_id(0)
    rows, inner = y_ref.shape
    width = c_ref.shape[1]
    groups = inner // width

    @pl.when(block == 0)
    def _():
        state = state_ref[...]
        top = state.astype(BF16)
        high[...] = top
        low[...] = (state - top.astype(F32)).astype(BF16)
        before[...] = jnp.zeros(before.shape, F32)

    cum = cum_ref[...] + before[0:1, :]
    before[...] = jnp.broadcast_to(cum[rows - 1 :, :], before.shape)
    reached = jnp.exp(cum)
    c = c_ref[...]
    lane = lane_ids((1, width))

    def half(gate_ref, first):
        def body(k, total):
            group = first + k
            at = pl.ds(pl.multiple_of(group * width, width), width)
            dot = lambda part: lax.dot_general(
                c, part[at, :], (((1,), (1,)), ((), ())), preferred_element_type=F32
            )
            carried = spread(reached, group * (width // head_dim) + lane // head_dim) * (
                dot(high) + dot(low)
            )
            gate = gate_ref[:, pl.ds(pl.multiple_of(k * width, width), width)].astype(F32)
            value = (y_ref[:, at] + carried) * (gate * jax.nn.sigmoid(gate))
            gated[:, at] = value
            return total + value * value

        return body

    total = jnp.zeros((rows, width), F32)
    total = lax.fori_loop(0, groups // 2, half(kept_ref, 0), total, unroll=5)
    total = lax.fori_loop(0, groups // 2, half(got_ref, groups // 2), total, unroll=5)
    scale = lax.rsqrt(jnp.sum(total, axis=1, keepdims=True) / inner + 1e-05)
    live = lax.broadcasted_iota(jnp.int32, (rows, 1), 0) + block * rows < scalars[1]
    shift = scalars[0] * (groups // 2)

    def write(group, _):
        at = pl.ds(pl.multiple_of(group * width, width), width)
        target = lax.rem(group + shift, groups)
        home = pl.ds(pl.multiple_of(target * width, width), width)
        value = gated[:, at] * scale * gain_ref[0:1, home]
        out_ref[:, home] = jnp.where(
            live, value, 0.0
        ).astype(BF16)
        return _

    lax.fori_loop(0, groups, write, 0, unroll=4)


def prefix_kernel(count, rows, head_dim, place_ref, got_ref, out_ref, turned):
    first = lax.div(place_ref[0] * rows, head_dim)
    edge = (first + 1) * head_dim - place_ref[0] * rows
    turned[...] = got_ref[:, rows, :].T
    shape = (rows, count)
    decays = jnp.exp(
        jnp.where(
            lax.broadcasted_iota(jnp.int32, shape, 0) < edge,
            jnp.broadcast_to(turned[pl.ds(first, 1), :], shape),
            jnp.broadcast_to(turned[pl.ds(first + 1, 1), :], shape),
        )
    )
    state = jnp.zeros((rows, got_ref.shape[2]), F32)
    for source in range(count):
        out_ref[source] = state
        if source < count - 1:
            factor = jnp.broadcast_to(decays[:, source : source + 1], state.shape)
            state = state * factor + got_ref[source, :rows, :]


def local(
    tokens, bounds, in_weight, conv_weight, conv_bias, dt_bias, decay_rate, skip_gain, norm_gain
):
    slots = tokens.shape[1]
    inner = norm_gain.shape[0]
    state_width = (conv_bias.shape[0] - inner) // 2
    heads = decay_rate.shape[0]
    head_dim = inner // heads
    kernel = conv_weight.shape[0]
    capacity = slots // BLOCK
    half = inner // 2
    core = lax.axis_index("fsdp")
    early_width = [4 * state_width] * 3
    early_total = sum(early_width)
    core_scalar = core.astype(jnp.int32)[None]
    part_shape = jax.ShapeDtypeStruct((in_weight.shape[0], early_total + half), BF16)
    kept_part, sent_part = pl.pallas_call(
        functools.partial(pack_kernel, inner, state_width),
        in_specs=[pl.BlockSpec(memory_space=pltpu.SMEM), pl.BlockSpec(memory_space=pltpu.VMEM)],
        out_specs=[pl.BlockSpec(memory_space=pltpu.VMEM)] * 2,
        out_shape=[part_shape] * 2,
        name="pack",
    )(core_scalar, in_weight)
    received = swapped(sent_part)
    shard = jnp.where(
        core == 0,
        jnp.concatenate([kept_part, received], axis=0),
        jnp.concatenate([received, kept_part], axis=0),
    )
    weight = lax.all_gather(shard, SEQ, axis=0, tiled=True)
    own_rows = tokens[0]
    shard_blocks = bounds[0, 0, 1] - bounds[0, 0, 0]
    edge = lax.dynamic_slice_in_dim(own_rows, shard_blocks * BLOCK - EDGE, EDGE, 0)
    own_all = jnp.concatenate([own_rows, passed_along(edge, SEQ, 1)], axis=0)
    other_all = swapped(own_all)

    def projected(rows, first, count):
        part = lax.slice_in_dim(weight, first, first + count, axis=1)
        return jnp.dot(rows, part, preferred_element_type=F32).astype(BF16)

    groups = inner // state_width
    scalars = jnp.stack([core.astype(jnp.int32), shard_blocks * BLOCK])
    bias_row, gain_row = conv_bias[None, :], norm_gain[None, :]
    dt_row, decay_row, skip_row = dt_bias[None, :], decay_rate[None, :], skip_gain[None, :]
    count = lax.axis_size(SEQ)
    chunk_rows = inner // count

    total_rows = slots + EDGE
    theirs = projected(other_all, 0, early_total)
    got = swapped(theirs)
    kept = projected(own_all, 0, early_total)
    last = groups // 2
    tile = lambda rows, index: pl.BlockSpec((rows, state_width), index)
    whole = lambda shape: pl.BlockSpec(shape, lambda *_: (0,) * len(shape))
    parts = 4
    wide = inner // parts
    turn = lambda p, c: lax.rem(p + c[0] * (parts // 2), parts)
    broad = lambda rows, index: pl.BlockSpec((rows, wide), index)
    xs, maps, cum, step, payload = pl.pallas_call(
        functools.partial(front_kernel, heads, head_dim, chunk_rows),
        grid_spec=pltpu.PrefetchScalarGridSpec(
            num_scalar_prefetch=1,
            grid=(parts,),
            in_specs=[
            broad(total_rows, lambda p, c: (0, jnp.minimum(p, parts // 2 - 1))),
            broad(total_rows, lambda p, c: (0, jnp.maximum(p - parts // 2, 0))),
            tile(total_rows, lambda g, c: (0, last)),
            tile(total_rows, lambda g, c: (0, last)),
            tile(total_rows, lambda g, c: (0, last + 1)),
            broad(kernel, lambda p, c: (0, turn(p, c))),
            broad(1, lambda p, c: (0, turn(p, c))),
            pl.BlockSpec((kernel, 2 * state_width), lambda g, c: (0, groups // 2)),
            pl.BlockSpec((1, 2 * state_width), lambda g, c: (0, groups // 2)),
            whole((1, heads)),
            whole((1, heads)),
        ],
        out_specs=[
            broad(slots, lambda p, c: (0, p)),
            whole((slots, 2 * state_width)),
            whole((slots, state_width)),
            whole((slots, state_width)),
            whole((count, chunk_rows + 8, state_width)),
        ],
            scratch_shapes=[
            pltpu.VMEM((groups // parts, total_rows, state_width), F32),
            pltpu.VMEM((slots, state_width), F32),
            pltpu.VMEM((state_width, slots), BF16),
            pltpu.VMEM((2, slots, state_width), BF16),
            pltpu.VMEM((2, slots, state_width), BF16),
        ],
        ),
        out_shape=[
            jax.ShapeDtypeStruct((slots, inner), BF16),
            jax.ShapeDtypeStruct((slots, 2 * state_width), BF16),
            jax.ShapeDtypeStruct((slots, state_width), F32),
            jax.ShapeDtypeStruct((slots, state_width), F32),
            jax.ShapeDtypeStruct((count, chunk_rows + 8, state_width), F32),
        ],
        cost_estimate=pl.CostEstimate(flops=4_000_000_000, bytes_accessed=12_000_000, transcendentals=4_000_000),
        name="front",
    )(scalars, kept, got, kept, got, kept, conv_weight, bias_row, conv_weight, bias_row, dt_row, decay_row)

    received = lax.all_to_all(payload, SEQ, 0, 0, tiled=True)
    block_tile = lambda columns, index: pl.BlockSpec((BLOCK, columns), index)
    y = pl.pallas_call(
        functools.partial(inner_kernel, head_dim, heads),
        grid=(capacity,),
        in_specs=[
            pl.BlockSpec(memory_space=pltpu.SMEM),
            block_tile(inner, lambda q: (q, 0)),
            block_tile(2 * state_width, lambda q: (q, 0)),
            block_tile(state_width, lambda q: (q, 0)),
            block_tile(state_width, lambda q: (q, 0)),
            whole((1, heads)),
        ],
        out_specs=block_tile(inner, lambda q: (q, 0)),
        out_shape=jax.ShapeDtypeStruct((slots, inner), F32),
        scratch_shapes=[
            pltpu.VMEM((groups, state_width, state_width), F32),
            pltpu.VMEM((BLOCK, BLOCK), F32),
            pltpu.VMEM((state_width, BLOCK), BF16),
            pltpu.VMEM((state_width, BLOCK), F32),
        ],
        cost_estimate=pl.CostEstimate(flops=20_000_000_000, bytes_accessed=14_000_000, transcendentals=12_000_000),
        name="inner",
    )(scalars, xs, maps, cum, step, skip_row)

    received, y = lax.optimization_barrier((received, y))
    before = pl.pallas_call(
        functools.partial(prefix_kernel, count, chunk_rows, head_dim),
        in_specs=[pl.BlockSpec(memory_space=pltpu.SMEM), pl.BlockSpec(memory_space=pltpu.VMEM)],
        out_specs=pl.BlockSpec(memory_space=pltpu.VMEM),
        out_shape=jax.ShapeDtypeStruct((count, chunk_rows, state_width), F32),
        scratch_shapes=[pltpu.VMEM((state_width, count), F32)],
        cost_estimate=pl.CostEstimate(flops=2_000_000_000, bytes_accessed=3_000_000, transcendentals=0),
        name="prefix",
    )(lax.axis_index(SEQ).astype(jnp.int32)[None], received)
    weight, _ = lax.optimization_barrier((weight, before))
    theirs_gate = project(other_all, weight, early_total, half)
    kept_gate = project(own_all, weight, early_total, half)
    got_gate = swapped(theirs_gate)

    state = lax.all_to_all(before, SEQ, 0, 0, tiled=True).reshape(inner, state_width)

    layer_out = pl.pallas_call(
        functools.partial(finish_kernel, head_dim),
        grid=(capacity,),
        in_specs=[
            pl.BlockSpec(memory_space=pltpu.SMEM),
            block_tile(half, lambda q: (q, 0)),
            block_tile(half, lambda q: (q, 0)),
            block_tile(inner, lambda q: (q, 0)),
            block_tile(state_width, lambda q: (q, 1)),
            block_tile(state_width, lambda q: (q, 0)),
            whole((inner, state_width)),
            whole((1, inner)),
        ],
        out_specs=block_tile(inner, lambda q: (q, 0)),
        out_shape=jax.ShapeDtypeStruct((slots, inner), BF16),
        scratch_shapes=[
            pltpu.VMEM((inner, state_width), BF16),
            pltpu.VMEM((inner, state_width), BF16),
            pltpu.VMEM((8, state_width), F32),
            pltpu.VMEM((BLOCK, inner), F32),
        ],
        cost_estimate=pl.CostEstimate(flops=4_000_000_000, bytes_accessed=18_000_000, transcendentals=4_000_000),
        name="finish",
    )(scalars, kept_gate, got_gate, y, maps, cum, state, gain_row)
    return layer_out[None]


def solution(mesh):
    split = Mesh(
        mesh.devices.reshape(4, 4, 4, mesh.shape["fsdp"]), ("seq_0", "seq_1", "seq_2", "fsdp")
    )
    return jax.shard_map(
        local,
        mesh=split,
        in_specs=(
            P("fsdp", SEQ, None),
            P("fsdp", SEQ, None),
            P(SEQ_FSDP, None),
            P(),
            P(),
            P(),
            P(),
            P(),
            P(),
        ),
        out_specs=P("fsdp", SEQ, None),
        check_vma=False,
    )
```

```python
import functools

import jax
import jax.numpy as jnp
from jax import lax
from jax.experimental import pallas as pl
from jax.experimental.pallas import tpu as pltpu
from jax.sharding import Mesh
from jax.sharding import PartitionSpec as P


BLOCK = 256
EDGE = 8
SEQ_FSDP = ("seq_0", "seq_1", "seq_2", "fsdp")
SEQ = ("seq_0", "seq_1", "seq_2")
F32 = jnp.float32
BF16 = jnp.bfloat16


def passed_along(value, axis, steps):
    count = lax.axis_size(axis)
    leading, last = (max(0, -steps), min(count, count - steps))
    return lax.ppermute(value, axis, [(source, source + steps) for source in range(leading, last)])


def swapped(value):
    return lax.ppermute(value, "fsdp", [(0, 1), (1, 0)])


def pack_kernel(inner, width, core_ref, weight_ref, kept_ref, sent_ref):
    half = inner // 2
    for which, target in ((core_ref[0], kept_ref), (1 - core_ref[0], sent_ref)):
        columns = lambda start, count: weight_ref[:, pl.ds(pl.multiple_of(start, 128), count)]
        target[:, :half] = columns(inner + half * which, half)
        target[:, half : half + width] = columns(2 * inner + width * which, width)
        steps = weight_ref.shape[1] - 2 * inner - 2 * width
        target[:, half + width : half + width + steps] = columns(2 * inner + 2 * width, steps)
        target[:, half + 2 * width :] = columns(half * which, half)


def project_kernel(rows_ref, weight_ref, out_ref):
    out_ref[...] = jnp.dot(
        rows_ref[...], weight_ref[...], preferred_element_type=F32
    ).astype(BF16)


def project(rows, weight, first, count):
    tile = 256
    return pl.pallas_call(
        project_kernel,
        grid=(count // tile,),
        in_specs=[
            pl.BlockSpec(memory_space=pltpu.VMEM),
            pl.BlockSpec((weight.shape[0], tile), lambda j: (0, first // tile + j)),
        ],
        out_specs=pl.BlockSpec((rows.shape[0], tile), lambda j: (0, j)),
        out_shape=jax.ShapeDtypeStruct((rows.shape[0], count), BF16),
        cost_estimate=pl.CostEstimate(
            flops=2 * rows.shape[0] * weight.shape[0] * count, bytes_accessed=14_000_000, transcendentals=0
        ),
        name="project_gate",
    )(rows, weight)


def split_dot(left, right, dims):
    high = right.astype(BF16)
    low = (right - high.astype(F32)).astype(BF16)
    dot = lambda part: lax.dot_general(left, part, (dims, ((), ())), preferred_element_type=F32)
    return dot(high) + dot(low)


def spread(table, lanes):
    index = jnp.broadcast_to(lanes, table.shape)
    return jnp.take_along_axis(table, index, axis=1)


def padded_row(ref, width):
    row = ref[...]
    return jnp.concatenate([row, jnp.zeros((1, width - row.shape[1]), row.dtype)], axis=1)


def lane_ids(shape):
    return lax.broadcasted_iota(jnp.int32, shape, 1)


def front_kernel(
    heads, head_dim, chunk_rows,
    scalars, kept_ref, got_ref, conv_ref, bias_ref, map_conv_ref, map_bias_ref, dt_ref, decay_ref,
    x_ref, maps_ref, cum_ref, step_ref, pay_ref,
    ext, factor, turned, high, low,
):
    part = pl.program_id(0)
    parts = pl.num_programs(0)
    slots, width = cum_ref.shape
    wide = x_ref.shape[1]
    inside, half = wide // width, wide * parts // 2
    chunk = 128

    def fill(ref, at, slot=0):
        ext[slot, :EDGE, :] = ref[slots:, at].astype(F32)
        ext[slot, EDGE:, :] = ref[:slots, at].astype(F32)

    def convolve(taps, bias, start, slot=0):
        first = EDGE - 3 + start
        total = bias + taps[0:1, :] * ext[slot, first : first + chunk, :]
        for offset in range(1, 4):
            total = total + taps[offset : offset + 1, :] * ext[slot, first + offset : first + offset + chunk, :]
        return (total * jax.nn.sigmoid(total)).astype(BF16)

    @pl.when(part == 0)
    def _():
        core, live = scalars[0], scalars[1]
        for which in range(2):
            taps = map_conv_ref[:, which * width : (which + 1) * width]
            bias = map_bias_ref[:, which * width : (which + 1) * width]

            @pl.when(core == which)
            def _():
                fill(kept_ref, pl.ds(half, width))

            @pl.when(core != which)
            def _():
                fill(got_ref, pl.ds(half, width))

            for start in range(0, slots, chunk):
                value = convolve(taps, bias, start)
                maps_ref[start : start + chunk, which * width : (which + 1) * width] = value
                if which == 0:
                    turned[:, start : start + chunk] = value.astype(F32).T.astype(BF16)
        lanes = lane_ids((slots, width))
        rows = lax.broadcasted_iota(jnp.int32, (slots, width), 0)
        turned_lanes = lane_ids((1, width)) + core * (heads // 2)
        turned_lanes = jnp.where(turned_lanes < heads, turned_lanes, turned_lanes - heads)
        turned_lanes = jnp.where(lane_ids((1, width)) < heads, turned_lanes, 0)
        row = lambda ref: spread(jnp.broadcast_to(padded_row(ref, width), (8, width)), turned_lanes)[0:1, :]
        shifted = spread(kept_ref[:slots, half + width : half + 2 * width].astype(F32), turned_lanes) + row(dt_ref)
        step = jnp.maximum(shifted, 0.0) + jnp.log1p(jnp.exp(-jnp.abs(shifted)))
        step = jnp.where((lanes < heads) & (rows < live), step, 0.0)
        step_ref[...] = step
        log_decay = -(step * jnp.where(lane_ids((1, width)) < heads, row(decay_ref), 0.0))
        triangle = (
            lax.broadcasted_iota(jnp.int32, (BLOCK, BLOCK), 0) >= lane_ids((BLOCK, BLOCK))
        ).astype(F32)
        before = jnp.zeros((1, width), F32)
        for lower in range(0, slots, BLOCK):
            cum = jnp.dot(
                triangle,
                log_decay[lower : lower + BLOCK],
                precision=lax.Precision.HIGHEST,
                preferred_element_type=F32,
            )
            cum_ref[lower : lower + BLOCK, :] = cum
            factor[lower : lower + BLOCK, :] = cum + before
            before = before + cum[BLOCK - 1 :, :]
        factor[...] = jnp.exp(before - factor[...]) * step
        pay_ref[:, chunk_rows:, :] = jnp.broadcast_to(
            before[None], (pay_ref.shape[0], pay_ref.shape[1] - chunk_rows, width)
        )

    @pl.when(part < parts // 2)
    def _():
        for k in range(inside):
            fill(kept_ref, pl.ds(pl.multiple_of(part * wide + k * width, width), width), k)

    @pl.when(part >= parts // 2)
    def _():
        for k in range(inside):
            fill(got_ref, pl.ds(pl.multiple_of((part - parts // 2) * wide + k * width, width), width), k)

    for k in range(inside):
        group = part * inside + k
        at = pl.ds(k * width, width)
        odd = k % 2

        lanes = group * (width // head_dim) + lane_ids((1, width)) // head_dim
        taps, bias = conv_ref[:, at], bias_ref[:, at]
        for start in range(0, slots, chunk):
            value = convolve(taps, bias, start, k)
            x_ref[start : start + chunk, at] = value
            weighted = value.astype(F32) * spread(factor[start : start + chunk, :], lanes)
            top = weighted.astype(BF16)
            high[odd, start : start + chunk, :] = top
            low[odd, start : start + chunk, :] = (weighted - top.astype(F32)).astype(BF16)
        state = jnp.dot(turned[...], high[odd], preferred_element_type=F32) + jnp.dot(
            turned[...], low[odd], preferred_element_type=F32
        )
        state = state.T
        pieces = chunk_rows // 8
        for r in range(width // 8):
            place = group * (width // 8) + r
            row = pl.multiple_of(lax.rem(place, pieces) * 8, 8)
            pay_ref[lax.div(place, pieces), pl.ds(row, 8), :] = state[8 * r : 8 * r + 8, :]


def inner_kernel(
    head_dim, heads,
    scalars, x_ref, maps_ref, cum_ref, step_ref, skip_ref, y_ref,
    run, scores, turned, across,
):
    block = pl.program_id(0)
    rows, width = cum_ref.shape
    part = rows // 2
    b, c = maps_ref[:, :width], maps_ref[:, width:]
    scores[...] = lax.dot_general(c, b, (((1,), (1,)), ((), ())), preferred_element_type=F32)
    turned[...] = b.astype(F32).T.astype(BF16)
    across[...] = (cum_ref[...] - jnp.log(step_ref[...])).T

    @pl.when(block == 0)
    def _():
        run[...] = jnp.zeros(run.shape, F32)

    lane = lane_ids((1, width))
    low_lanes = lane_ids((rows, width)) < head_dim
    causal = lax.broadcasted_iota(jnp.int32, (part, part), 0) >= lane_ids((part, part))
    skips = jnp.broadcast_to(padded_row(skip_ref, width), (8, width))

    def each(group, carry):
        at = pl.ds(pl.multiple_of(group * width, width), width)
        first_head = group * (width // head_dim)
        cum = cum_ref[...]
        by_head = [spread(cum, jnp.zeros((1, width), jnp.int32) + first_head + e) for e in range(2)]
        cum_x = jnp.where(low_lanes, by_head[0], by_head[1])
        step_x = spread(step_ref[...], first_head + lane // head_dim)
        x = x_ref[:, at]
        outs = []
        for e in range(2):
            row = across[pl.ds(first_head + e, 1), :]
            column = by_head[e]

            def mixing(i, j):
                exponent = column[i * part : (i + 1) * part, :] - row[:, j * part : (j + 1) * part]
                if i == j:
                    exponent = jnp.where(causal, exponent, -jnp.inf)
                value = jnp.exp(exponent) * scores[i * part : (i + 1) * part, j * part : (j + 1) * part]
                top = value.astype(BF16)
                return top, (value - top.astype(F32)).astype(BF16)

            m00, m10, m11 = mixing(0, 0), mixing(1, 0), mixing(1, 1)
            dot = lambda m, j: jnp.dot(m, x[j * part : (j + 1) * part], preferred_element_type=F32)
            outs.append(
                jnp.concatenate(
                    [
                        dot(m00[0], 0) + dot(m00[1], 0),
                        (dot(m10[0], 0) + dot(m10[1], 0)) + (dot(m11[0], 1) + dot(m11[1], 1)),
                    ],
                    axis=0,
                )
            )
        x32 = x.astype(F32)
        turned_head = first_head + scalars[0] * (heads // 2)
        turned_head = jnp.where(turned_head < heads, turned_head, turned_head - heads)
        skip = spread(skips, turned_head + lane // head_dim)
        state = run[group]
        reach = split_dot(maps_ref[:, width:], state, ((1,), (0,)))
        y_ref[:, at] = (
            jnp.where(low_lanes, outs[0], outs[1]) + jnp.exp(cum_x) * reach + skip[0:1, :] * x32
        )
        end = cum_x[rows - 1 :, :]
        weighted = x32 * (jnp.exp(end - cum_x) * step_x)
        run[group] = jnp.exp(end) * state + split_dot(turned[...], weighted, ((1,), (0,)))
        return carry

    lax.fori_loop(0, run.shape[0], each, 0, unroll=4)


def finish_kernel(
    head_dim,
    scalars, kept_ref, got_ref, y_ref, c_ref, cum_ref, state_ref, gain_ref, out_ref,
    high, low, before, gated,
):
    block = pl.program_id(0)
    rows, inner = y_ref.shape
    width = c_ref.shape[1]
    groups = inner // width

    @pl.when(block == 0)
    def _():
        state = state_ref[...]
        top = state.astype(BF16)
        high[...] = top
        low[...] = (state - top.astype(F32)).astype(BF16)
        before[...] = jnp.zeros(before.shape, F32)

    cum = cum_ref[...] + before[0:1, :]
    before[...] = jnp.broadcast_to(cum[rows - 1 :, :], before.shape)
    reached = jnp.exp(cum)
    c = c_ref[...]
    lane = lane_ids((1, width))

    def half(gate_ref, first):
        def body(k, total):
            group = first + k
            at = pl.ds(pl.multiple_of(group * width, width), width)
            dot = lambda part: lax.dot_general(
                c, part[at, :], (((1,), (1,)), ((), ())), preferred_element_type=F32
            )
            carried = spread(reached, group * (width // head_dim) + lane // head_dim) * (
                dot(high) + dot(low)
            )
            gate = gate_ref[:, pl.ds(pl.multiple_of(k * width, width), width)].astype(F32)
            value = (y_ref[:, at] + carried) * (gate * jax.nn.sigmoid(gate))
            gated[:, at] = value
            return total + value * value

        return body

    total = jnp.zeros((rows, width), F32)
    total = lax.fori_loop(0, groups // 2, half(kept_ref, 0), total, unroll=5)
    total = lax.fori_loop(0, groups // 2, half(got_ref, groups // 2), total, unroll=5)
    scale = lax.rsqrt(jnp.sum(total, axis=1, keepdims=True) / inner + 1e-05)
    live = lax.broadcasted_iota(jnp.int32, (rows, 1), 0) + block * rows < scalars[1]
    shift = scalars[0] * (groups // 2)

    def write(group, _):
        at = pl.ds(pl.multiple_of(group * width, width), width)
        target = lax.rem(group + shift, groups)
        home = pl.ds(pl.multiple_of(target * width, width), width)
        value = gated[:, at] * scale * gain_ref[0:1, home]
        out_ref[:, home] = jnp.where(
            live, value, 0.0
        ).astype(BF16)
        return _

    lax.fori_loop(0, groups, write, 0, unroll=4)


def prefix_kernel(count, rows, head_dim, place_ref, got_ref, out_ref, turned):
    first = lax.div(place_ref[0] * rows, head_dim)
    edge = (first + 1) * head_dim - place_ref[0] * rows
    turned[...] = got_ref[:, rows, :].T
    shape = (rows, count)
    decays = jnp.exp(
        jnp.where(
            lax.broadcasted_iota(jnp.int32, shape, 0) < edge,
            jnp.broadcast_to(turned[pl.ds(first, 1), :], shape),
            jnp.broadcast_to(turned[pl.ds(first + 1, 1), :], shape),
        )
    )
    state = jnp.zeros((rows, got_ref.shape[2]), F32)
    for source in range(count):
        out_ref[source] = state
        if source < count - 1:
            factor = jnp.broadcast_to(decays[:, source : source + 1], state.shape)
            state = state * factor + got_ref[source, :rows, :]


def local(
    tokens, bounds, in_weight, conv_weight, conv_bias, dt_bias, decay_rate, skip_gain, norm_gain
):
    slots = tokens.shape[1]
    inner = norm_gain.shape[0]
    state_width = (conv_bias.shape[0] - inner) // 2
    heads = decay_rate.shape[0]
    head_dim = inner // heads
    kernel = conv_weight.shape[0]
    capacity = slots // BLOCK
    half = inner // 2
    core = lax.axis_index("fsdp")
    early_width = [4 * state_width] * 3
    early_total = sum(early_width)
    core_scalar = core.astype(jnp.int32)[None]
    part_shape = jax.ShapeDtypeStruct((in_weight.shape[0], early_total + half), BF16)
    kept_part, sent_part = pl.pallas_call(
        functools.partial(pack_kernel, inner, state_width),
        in_specs=[pl.BlockSpec(memory_space=pltpu.SMEM), pl.BlockSpec(memory_space=pltpu.VMEM)],
        out_specs=[pl.BlockSpec(memory_space=pltpu.VMEM)] * 2,
        out_shape=[part_shape] * 2,
        name="pack",
    )(core_scalar, in_weight)
    received = swapped(sent_part)
    shard = jnp.where(
        core == 0,
        jnp.concatenate([kept_part, received], axis=0),
        jnp.concatenate([received, kept_part], axis=0),
    )
    weight = lax.all_gather(shard, SEQ, axis=0, tiled=True)
    own_rows = tokens[0]
    shard_blocks = bounds[0, 0, 1] - bounds[0, 0, 0]
    edge = lax.dynamic_slice_in_dim(own_rows, shard_blocks * BLOCK - EDGE, EDGE, 0)
    own_all = jnp.concatenate([own_rows, passed_along(edge, SEQ, 1)], axis=0)
    other_all = swapped(own_all)

    def projected(rows, first, count):
        part = lax.slice_in_dim(weight, first, first + count, axis=1)
        return jnp.dot(rows, part, preferred_element_type=F32).astype(BF16)

    groups = inner // state_width
    scalars = jnp.stack([core.astype(jnp.int32), shard_blocks * BLOCK])
    bias_row, gain_row = conv_bias[None, :], norm_gain[None, :]
    dt_row, decay_row, skip_row = dt_bias[None, :], decay_rate[None, :], skip_gain[None, :]
    own_all, bias_row, gain_row, scalars = lax.optimization_barrier(
        (own_all, bias_row, gain_row, scalars)
    )
    count = lax.axis_size(SEQ)
    chunk_rows = inner // count

    total_rows = slots + EDGE
    theirs = projected(other_all, 0, early_total)
    got = swapped(theirs)
    kept = projected(own_all, 0, early_total)
    whole = lambda shape: pl.BlockSpec(shape, lambda *_: (0,) * len(shape))
    parts = 4
    wide = inner // parts
    turn = lambda p, c: lax.rem(p + c[0] * (parts // 2), parts)
    broad = lambda rows, index: pl.BlockSpec((rows, wide), index)
    xs, maps, cum, step, payload = pl.pallas_call(
        functools.partial(front_kernel, heads, head_dim, chunk_rows),
        grid_spec=pltpu.PrefetchScalarGridSpec(
            num_scalar_prefetch=1,
            grid=(parts,),
            in_specs=[
            pl.BlockSpec(memory_space=pltpu.VMEM),
            pl.BlockSpec(memory_space=pltpu.VMEM),
            broad(kernel, lambda p, c: (0, turn(p, c))),
            broad(1, lambda p, c: (0, turn(p, c))),
            pl.BlockSpec((kernel, 2 * state_width), lambda g, c: (0, groups // 2)),
            pl.BlockSpec((1, 2 * state_width), lambda g, c: (0, groups // 2)),
            whole((1, heads)),
            whole((1, heads)),
        ],
        out_specs=[
            broad(slots, lambda p, c: (0, p)),
            whole((slots, 2 * state_width)),
            whole((slots, state_width)),
            whole((slots, state_width)),
            whole((count, chunk_rows + 8, state_width)),
        ],
            scratch_shapes=[
            pltpu.VMEM((groups // parts, total_rows, state_width), F32),
            pltpu.VMEM((slots, state_width), F32),
            pltpu.VMEM((state_width, slots), BF16),
            pltpu.VMEM((2, slots, state_width), BF16),
            pltpu.VMEM((2, slots, state_width), BF16),
        ],
        ),
        out_shape=[
            jax.ShapeDtypeStruct((slots, inner), BF16),
            jax.ShapeDtypeStruct((slots, 2 * state_width), BF16),
            jax.ShapeDtypeStruct((slots, state_width), F32),
            jax.ShapeDtypeStruct((slots, state_width), F32),
            jax.ShapeDtypeStruct((count, chunk_rows + 8, state_width), F32),
        ],
        cost_estimate=pl.CostEstimate(flops=4_000_000_000, bytes_accessed=12_000_000, transcendentals=4_000_000),
        compiler_params=pltpu.CompilerParams(vmem_limit_bytes=44 * 1024 * 1024),
        name="front",
    )(scalars, kept, got, conv_weight, bias_row, conv_weight, bias_row, dt_row, decay_row)

    received = lax.all_to_all(payload, SEQ, 0, 0, tiled=True)
    block_tile = lambda columns, index: pl.BlockSpec((BLOCK, columns), index)
    y = pl.pallas_call(
        functools.partial(inner_kernel, head_dim, heads),
        grid=(capacity,),
        in_specs=[
            pl.BlockSpec(memory_space=pltpu.SMEM),
            block_tile(inner, lambda q: (q, 0)),
            block_tile(2 * state_width, lambda q: (q, 0)),
            block_tile(state_width, lambda q: (q, 0)),
            block_tile(state_width, lambda q: (q, 0)),
            whole((1, heads)),
        ],
        out_specs=block_tile(inner, lambda q: (q, 0)),
        out_shape=jax.ShapeDtypeStruct((slots, inner), F32),
        scratch_shapes=[
            pltpu.VMEM((groups, state_width, state_width), F32),
            pltpu.VMEM((BLOCK, BLOCK), F32),
            pltpu.VMEM((state_width, BLOCK), BF16),
            pltpu.VMEM((state_width, BLOCK), F32),
        ],
        cost_estimate=pl.CostEstimate(flops=20_000_000_000, bytes_accessed=14_000_000, transcendentals=12_000_000),
        name="inner",
    )(scalars, xs, maps, cum, step, skip_row)

    received, y = lax.optimization_barrier((received, y))
    before = pl.pallas_call(
        functools.partial(prefix_kernel, count, chunk_rows, head_dim),
        in_specs=[pl.BlockSpec(memory_space=pltpu.SMEM), pl.BlockSpec(memory_space=pltpu.VMEM)],
        out_specs=pl.BlockSpec(memory_space=pltpu.VMEM),
        out_shape=jax.ShapeDtypeStruct((count, chunk_rows, state_width), F32),
        scratch_shapes=[pltpu.VMEM((state_width, count), F32)],
        cost_estimate=pl.CostEstimate(flops=2_000_000_000, bytes_accessed=3_000_000, transcendentals=0),
        compiler_params=pltpu.CompilerParams(vmem_limit_bytes=10 * 1024 * 1024),
        name="prefix",
    )(lax.axis_index(SEQ).astype(jnp.int32)[None], received)
    weight, _ = lax.optimization_barrier((weight, before))
    theirs_gate = project(other_all, weight, early_total, half)
    kept_gate = project(own_all, weight, early_total, half)
    got_gate = swapped(theirs_gate)

    state = lax.all_to_all(before, SEQ, 0, 0, tiled=True).reshape(inner, state_width)

    layer_out = pl.pallas_call(
        functools.partial(finish_kernel, head_dim),
        grid=(capacity,),
        in_specs=[
            pl.BlockSpec(memory_space=pltpu.SMEM),
            block_tile(half, lambda q: (q, 0)),
            block_tile(half, lambda q: (q, 0)),
            block_tile(inner, lambda q: (q, 0)),
            block_tile(state_width, lambda q: (q, 1)),
            block_tile(state_width, lambda q: (q, 0)),
            pl.BlockSpec(memory_space=pltpu.VMEM),
            whole((1, inner)),
        ],
        out_specs=block_tile(inner, lambda q: (q, 0)),
        out_shape=jax.ShapeDtypeStruct((slots, inner), BF16),
        scratch_shapes=[
            pltpu.VMEM((inner, state_width), BF16),
            pltpu.VMEM((inner, state_width), BF16),
            pltpu.VMEM((8, state_width), F32),
            pltpu.VMEM((BLOCK, inner), F32),
        ],
        cost_estimate=pl.CostEstimate(flops=4_000_000_000, bytes_accessed=18_000_000, transcendentals=4_000_000),
        name="finish",
    )(scalars, kept_gate, got_gate, y, maps, cum, state, gain_row)
    return layer_out[None]


def solution(mesh):
    split = Mesh(
        mesh.devices.reshape(4, 4, 4, mesh.shape["fsdp"]), ("seq_0", "seq_1", "seq_2", "fsdp")
    )
    return jax.shard_map(
        local,
        mesh=split,
        in_specs=(
            P("fsdp", SEQ, None),
            P("fsdp", SEQ, None),
            P(SEQ_FSDP, None),
            P(),
            P(),
            P(),
            P(),
            P(),
            P(),
        ),
        out_specs=P("fsdp", SEQ, None),
        check_vma=False,
    )
```
